32 devices in a mesh: dp: 16 (over z, x, core), tensor: 2 (over y).
Axes of the slice: x: 2, y: 2, z: 4, core: 2. Of those that a mesh axis runs over, the one named last changes fastest.
Arguments:
- latents: bfloat16 [16, 1024, 1152], P('dp', 'tensor'), may hold values from -1.6953125 to 1.6953125
- timestep: float32 [16, 6, 1152], P('dp'), may hold values from -0.5 to 0.5
- text: bfloat16 [16, 120, 1152], P('dp'), may hold values from -1.6953125 to 1.6953125
- lengths: int32 [16], P('dp'), may hold values from 1 to 120
- table: float32 [6, 1152], replicated, may hold values from -0.5 to 0.5
- w_qkv: bfloat16 [1152, 3, 1152], P('dp', None, 'tensor'), may hold values from -0.1875 to 0.1875
- b_qv: float32 [2, 1152], replicated, may hold values from -0.5 to 0.5
- w_proj: bfloat16 [1152, 1152], P('dp', 'tensor'), may hold values from -0.75 to 0.75
- w_cq: bfloat16 [1152, 1152], P('dp', 'tensor'), may hold values from -0.1875 to 0.1875
- w_ckv: bfloat16 [1152, 2, 1152], P('dp', None, 'tensor'), may hold values from -0.1875 to 0.1875
- b_cqv: float32 [2, 1152], replicated, may hold values from -0.5 to 0.5
- w_cproj: bfloat16 [1152, 1152], P('dp', 'tensor'), may hold values from -0.375 to 0.375
- w_fc1: bfloat16 [1152, 4608], P('dp', 'tensor'), may hold values from -0.1875 to 0.1875
- b_fc1: float32 [4608], replicated, may hold values from -0.5 to 0.5
- w_fc2: bfloat16 [1152, 4608], P('dp', 'tensor'), may hold values from -0.09375 to 0.09375
- b_out: float32 [3, 1152], replicated, may hold values from -0.5 to 0.5
- cotangent: bfloat16 [16, 1024, 1152], P('dp', 'tensor'), may hold values from -6 to 6
Outputs:
- block_out: float32 [16, 1024, 1152], P('dp', 'tensor')
- latents_grad: float32 [16, 1024, 1152], P('dp', 'tensor')
- timestep_grad: float32 [16, 6, 1152], P('dp', None, 'tensor')
- text_grad: float32 [16, 120, 1152], P('dp', None, 'tensor')
- table_grad: float32 [6, 1152], replicated
- w_qkv_grad: float32 [1152, 3, 1152], P('dp', None, 'tensor')
- b_qv_grad: float32 [2, 1152], replicated
- w_proj_grad: float32 [1152, 1152], P('dp', 'tensor')
- w_cq_grad: float32 [1152, 1152], P('dp', 'tensor')
- w_ckv_grad: float32 [1152, 2, 1152], P('dp', None, 'tensor')
- b_cqv_grad: float32 [2, 1152], replicated
- w_cproj_grad: float32 [1152, 1152], P('dp', 'tensor')
- w_fc1_grad: float32 [1152, 4608], P('dp', 'tensor')
- b_fc1_grad: float32 [4608], replicated
- w_fc2_grad: float32 [1152, 4608], P('dp', 'tensor')
- b_out_grad: float32 [3, 1152], replicated
The draws below stay inside these ranges and needn't reach their ends.
Inputs may be any that keep to these rules, and one draw needn't show every extreme that they name: The first lengths[b] caption tokens of latent b are real, the rest padding.
All inputs are finite; a program needn't handle non-finite values.
Results may differ from the reference program's by a relative error of at most 0.014.
Values may be sent and summed in bfloat16 or wider, within the bound.
A program may use at most 256 MiB of HBM per device.

```python
import math
import jax
import jax.numpy as jnp
from jax import lax

D = 1152
HEADS = 16
FF = 4608
TEXT = 120
SEQ = 1024
HEAD = 72
BATCH = 16


def touch_ends(drawn, rng, low, largest):
    shape = drawn.shape
    spot = [jax.random.randint(jax.random.fold_in(rng, axis), (), 0, shape[axis]) for axis in range(len(shape))]
    drawn = drawn.at[tuple(spot)].set(low)
    longest = shape.index(max(shape))
    spot[longest] = (spot[longest] + 1) % shape[longest]
    return drawn.at[tuple(spot)].set(largest)


def spiked(drawn, stream_key, source, target, parts, factor):
    owner, partner = [(jnp.arange(drawn.shape[axis_at]) // (drawn.shape[axis_at] // parts)).reshape([-1 if axis == axis_at else 1 for axis in range(drawn.ndim)]) for axis_at in (source, target)]
    chosen = jax.random.permutation(stream_key, parts)[partner]
    strong = (owner == chosen) | (owner == (partner + parts // 2) % parts)
    return jnp.where(strong, factor * drawn, drawn)


def shard_levels(key, extent, shards, smallest, largest):
    def one(axis_at, parts):
        draws = jax.random.uniform(jax.random.fold_in(jax.random.fold_in(key, 6), axis_at), (parts,), jnp.float32, smallest / len(shards), largest / len(shards))
        return jnp.repeat(jnp.exp(draws), extent[axis_at] // parts).reshape((-1,) + (1,) * (len(extent) - axis_at - 1))

    gain = one(*shards[0])
    for cut in shards[1:]:
        gain = gain * one(*cut)
    return gain


def bell_draw(key, shape, scale, limit, shards=(), held_as=jnp.bfloat16):
    array = jax.random.normal(key, shape, jnp.float32) * scale
    if len(shards) > 0:
        array = shard_levels(key, shape, shards, -0.22, 0.18) * array
    return jnp.clip(array, min=-limit, max=limit).astype(held_as)


def heavy_noise(key, extent, width, reach, split, heavy, held_as=jnp.bfloat16):
    values = width * jax.random.normal(key, extent, jnp.float32)
    if split:
        values = values * shard_levels(key, extent, split, -0.22, 0.18)
    return jnp.clip(spiked(values, jax.random.fold_in(key, 3), *heavy), -reach, reach).astype(held_as)


def setup_inputs(seed: int = 0) -> dict:
    seeds = jax.random.split(jax.random.key(seed), 18)
    return {
        "latents": jnp.clip(jax.random.uniform(seeds[0], (BATCH, SEQ, D), jnp.float32, -1.6953125, 1.6953125) * shard_levels(seeds[0], (BATCH, SEQ, D), ((0, 16), (1, 2)), -0.4, 0.0), -1.6953125, 1.6953125).astype(jnp.bfloat16),
        "timestep": jnp.clip(jax.random.uniform(seeds[1], (BATCH, 6, D), jnp.float32, -0.5, 0.5) * shard_levels(seeds[1], (BATCH, 6, D), ((0, 16),), -0.4, 0.0), -0.5, 0.5),
        "text": jnp.clip(jax.random.uniform(seeds[2], (BATCH, TEXT, D), jnp.float32, -1.6953125, 1.6953125) * shard_levels(seeds[2], (BATCH, TEXT, D), ((0, 16),), -0.4, 0.0), -1.6953125, 1.6953125).astype(jnp.bfloat16),
        "lengths": touch_ends(jax.random.randint(seeds[3], (BATCH,), 1, TEXT + 1), jax.random.fold_in(seeds[3], 1), 1, TEXT).astype(jnp.int32),
        "table": jnp.clip(jax.random.uniform(seeds[4], (6, D), jnp.float32, -0.5, 0.5), -0.5, 0.5),
        "w_qkv": bell_draw(seeds[5], (D, 3, D), D ** -0.5, 0.1875, ((0, 16), (2, 2))),
        "b_qv": jnp.clip(jax.random.uniform(seeds[6], (2, D), jnp.float32, -0.5, 0.5), -0.5, 0.5),
        "w_proj": bell_draw(seeds[7], (D, D), (D // 16) ** -0.5, 0.75, ((0, 16), (1, 2))),
        "w_cq": bell_draw(seeds[8], (D, D), D ** -0.5, 0.1875, ((0, 16), (1, 2))),
        "w_ckv": bell_draw(seeds[9], (D, 2, D), D ** -0.5, 0.1875, ((0, 16), (2, 2))),
        "b_cqv": jnp.clip(jax.random.uniform(seeds[10], (2, D), jnp.float32, -0.5, 0.5), -0.5, 0.5),
        "w_cproj": bell_draw(seeds[11], (D, D), (D // 4) ** -0.5, 0.375, ((0, 16), (1, 2))),
        "w_fc1": bell_draw(seeds[12], (D, FF), D ** -0.5, 0.1875, ((0, 16), (1, 2))),
        "b_fc1": jnp.clip(jax.random.uniform(seeds[13], (FF,), jnp.float32, -0.5, 0.5), -0.5, 0.5),
        "w_fc2": bell_draw(seeds[14], (D, FF), FF ** -0.5, 0.09375, ((0, 16), (1, 2))),
        "b_out": jnp.clip(jax.random.uniform(seeds[15], (3, D), jnp.float32, -0.5, 0.5), -0.5, 0.5),
        "cotangent": heavy_noise(seeds[16], (BATCH, SEQ, D), 1.0, 6.0, ((0, 16), (1, 2)), (0, 2, 16, 2.0)),
    }


highest = lax.Precision.HIGHEST
epsilon = 1e-06

@jax.custom_vjp
def low(v):
    return lax.optimization_barrier(v.astype(jnp.bfloat16)).astype(jnp.float32)

@jax.custom_vjp
def low_back(v):
    return v

def low_keep(v):
    return (low(v), None)

def low_pass(kept, grad):
    return (grad,)

def back_keep(v):
    return (v, None)

def back_low(kept, grad):
    return (low(grad),)
low.defvjp(low_keep, low_pass)
low_back.defvjp(back_keep, back_low)

def round_both(values):
    return low(low_back(values))

def layer_norm(values):
    row_mean = lax.optimization_barrier(jnp.mean(values, axis=-1, keepdims=True))
    centred = values - row_mean
    spread = lax.optimization_barrier(jnp.mean(centred * centred, axis=-1, keepdims=True))
    return centred * lax.rsqrt(spread + epsilon)

def softmax_rows(scores):
    peak = lax.optimization_barrier(jnp.max(scores, axis=-1, keepdims=True))
    weights = jnp.exp(scores - peak)
    return weights / lax.optimization_barrier(jnp.sum(weights, axis=-1, keepdims=True))

def gelu_tanh(values):
    return jax.nn.gelu(values, approximate=True)

def matmul(left_rows, right_rows):
    return jnp.dot(left_rows, right_rows, precision=highest, preferred_element_type=jnp.float32)

def project_back(row_payload, weight_matrix):
    return matmul(row_payload, weight_matrix.T)

def diffusion_transformer_block(latent_tokens, timestep_row, caption_tokens, key_validity_mask, block_parameters):
    table, w_qkv, b_qv, w_proj, w_cq, w_ckv, b_cqv, w_cproj, w_fc1, b_fc1, w_fc2, b_out = block_parameters
    modulation = table + timestep_row
    scale_root = 1.0 / math.sqrt(HEAD)
    normed_self = low(layer_norm(latent_tokens) * (1.0 + modulation[1]) + modulation[0])
    query_rows = round_both(matmul(normed_self, w_qkv[:, 0]) + b_qv[0])
    key_rows = round_both(matmul(normed_self, w_qkv[:, 1]))
    value_rows = round_both(matmul(normed_self, w_qkv[:, 2]) + b_qv[1])
    query_heads = query_rows.reshape(SEQ, HEADS, HEAD)
    key_heads = key_rows.reshape(SEQ, HEADS, HEAD)
    value_heads = value_rows.reshape(SEQ, HEADS, HEAD)
    scores = low_back(jnp.einsum('qhe,khe->hqk', query_heads, key_heads, precision=highest) * scale_root)
    attn_probs = low(softmax_rows(scores))
    mixture = round_both(jnp.einsum('hqk,khe->qhe', attn_probs, value_heads, precision=highest).reshape(SEQ, D))
    attn_out = low_back(project_back(mixture, w_proj)) + b_out[0]
    after_self = latent_tokens + modulation[2] * attn_out
    cross_in = low(after_self)
    c_query = round_both(matmul(cross_in, w_cq) + b_cqv[0]).reshape(SEQ, HEADS, HEAD)
    c_key = round_both(matmul(caption_tokens, w_ckv[:, 0])).reshape(TEXT, HEADS, HEAD)
    c_value = round_both(matmul(caption_tokens, w_ckv[:, 1]) + b_cqv[1]).reshape(TEXT, HEADS, HEAD)
    c_scores = low_back(jnp.einsum('qhe,khe->hqk', c_query, c_key, precision=highest) * scale_root)
    c_scores = jnp.where(key_validity_mask[None, None, :], c_scores, -1000000000.0)
    c_probs = low(softmax_rows(c_scores))
    c_mixed = round_both(jnp.einsum('hqk,khe->qhe', c_probs, c_value, precision=highest).reshape(SEQ, D))
    cross_out = low_back(project_back(c_mixed, w_cproj)) + b_out[1]
    after_cross = after_self + cross_out
    normed_mlp = low(layer_norm(after_cross) * (1.0 + modulation[4]) + modulation[3])
    pre_act = low_back(matmul(normed_mlp, w_fc1) + b_fc1)
    active = low(gelu_tanh(pre_act))
    mlp_out = low_back(project_back(active, w_fc2)) + b_out[2]
    return after_cross + modulation[5] * mlp_out

def reference(latents, timestep, text, lengths, table, w_qkv, b_qv, w_proj, w_cq, w_ckv, b_cqv, w_cproj, w_fc1, b_fc1, w_fc2, b_out, cotangent):
    block_parameters = (table, w_qkv.astype(jnp.float32), b_qv, w_proj.astype(jnp.float32), w_cq.astype(jnp.float32), w_ckv.astype(jnp.float32), b_cqv, w_cproj.astype(jnp.float32), w_fc1.astype(jnp.float32), b_fc1, w_fc2.astype(jnp.float32), b_out)
    positions = jnp.arange(TEXT, dtype=jnp.int32)
    zero_grads = jax.tree.map(jnp.zeros_like, block_parameters)

    def scan_step(running, per_latent):
        latent_tokens, timestep_row, caption_tokens, length, upstream = per_latent
        key_validity_mask = positions < length

        def forward(latent_input, timestep_input, caption_input, parameters_input):
            return diffusion_transformer_block(latent_input, timestep_input, caption_input, key_validity_mask, parameters_input)
        block_out, pullback = jax.vjp(forward, latent_tokens.astype(jnp.float32), timestep_row, caption_tokens.astype(jnp.float32), block_parameters)
        grad_latent, grad_stamp, grad_caption, grad_params = pullback(upstream.astype(jnp.float32))
        running = jax.tree.map(jnp.add, running, grad_params)
        return (running, (block_out, grad_latent, grad_stamp, grad_caption))
    totals, stacked = lax.scan(scan_step, zero_grads, (latents, timestep, text, lengths, cotangent))
    block_out, grad_latents, grad_stamps, grad_text = stacked
    return (block_out, grad_latents, grad_stamps, grad_text, totals[0], totals[1], totals[2], totals[3], totals[4], totals[5], totals[6], totals[7], totals[8], totals[9], totals[10], totals[11])
```

```python
import math

import jax
import jax.numpy as jnp
from jax import lax
from jax.experimental import pallas as pl
from jax.experimental.pallas import tpu as pltpu
from jax.sharding import PartitionSpec as P
BF=jnp.bfloat16; F32=jnp.float32
MESH=pl.DeviceIdType.MESH
ANY=pl.BlockSpec(memory_space=pl.ANY)

def place(sizes):
    d=lax.axis_index("dp")
    return {"t": lax.axis_index("tensor"), "z": d//4, "x": (d//2)%2, "c": d%2}

def device(at):
    return {"dp": (at["z"]*2+at["x"])*2+at["c"], "tensor": at["t"]}

def peer(at, sizes, axis, step):
    other=dict(at)
    other[axis]=lax.rem(at[axis]+step, sizes[axis])
    return other

def greet(at, sizes):
    barrier=pltpu.get_barrier_semaphore()
    count=0
    for axis in "tzxc":
        for step in range(1,sizes[axis]):
            pl.semaphore_signal(barrier,inc=1,device_id=device(peer(at,sizes,axis,step)),device_id_type=MESH)
            count+=1
    pl.semaphore_wait(barrier,count)

def region(at, full):
    return tuple(slice(None) if axis in full else at[axis] for axis in "tzxc")

def gather_kernel(*refs, sizes, orders):
    n=len(orders)
    shards,outs=refs[:n],refs[n:2*n]
    own_sem,send_sem,recv_sem=refs[2*n:]
    at=place(sizes)
    greet(at,sizes)
    def copies(b,phase):
        axis=orders[b][phase]
        full=orders[b][:phase]
        made=[]
        for step in range(1,sizes[axis]):
            part=outs[b].at[region(at,full)]
            made.append(pltpu.make_async_remote_copy(
                src_ref=shards[b] if phase==0 else part, dst_ref=part,
                send_sem=send_sem.at[b,phase,step-1], recv_sem=recv_sem.at[b,phase,step-1],
                device_id=device(peer(at,sizes,axis,step)), device_id_type=MESH))
        return made
    own=[pltpu.make_async_copy(shards[b],outs[b].at[region(at,"")],own_sem.at[b]) for b in range(n)]
    begun=[]
    def start(b,phase):
        for cp in copies(b,phase):
            cp.start(); begun.append(cp)
    def arrive(b,phase):
        for cp in copies(b,phase): cp.wait_recv()
    for b in range(n): own[b].start()
    for b in range(n): start(b,0)
    pairs=[range(b,min(b+2,n)) for b in range(0,n,2)]
    for k,pair in enumerate(pairs):
        for b in pair:
            own[b].wait(); arrive(b,0); start(b,1)
        for b in pair:
            arrive(b,1); start(b,2)
        if k>0:
            for b in pairs[k-1]:
                arrive(b,2); start(b,3)
    for b in pairs[-1]:
        arrive(b,2); start(b,3)
    for b in range(n): arrive(b,3)
    for cp in begun: cp.wait_send()

def gather(blocks, sizes, orders, cid):
    n=len(blocks)
    r,cols=blocks[0].shape
    most=max(sizes.values())-1
    return pl.pallas_call(
        lambda *refs: gather_kernel(*refs,sizes=sizes,orders=orders),
        in_specs=[pl.BlockSpec(memory_space=pltpu.VMEM)]*n, out_specs=[ANY]*n,
        out_shape=[jax.ShapeDtypeStruct((sizes["t"],sizes["z"],sizes["x"],sizes["c"])+b.shape,b.dtype) for b in blocks],
        scratch_shapes=[pltpu.SemaphoreType.DMA((n,)),pltpu.SemaphoreType.DMA((n,4,most)),pltpu.SemaphoreType.DMA((n,4,most))],
        compiler_params=pltpu.CompilerParams(collective_id=cid,has_side_effects=True,vmem_limit_bytes=32<<20),
        name="gather_rows")(*blocks)

def reduce_kernel(*refs, sizes, orders):
    n=len(orders); T=sizes["t"]; Z=sizes["z"]; X=sizes["x"]
    grads=[refs[b*T:(b+1)*T] for b in range(n)]
    refs=refs[n*T:]
    outs=refs[:n]
    own=refs[n]; held=refs[n+1:2*n+1]; got=[refs[2*n+1+3*b:2*n+4+3*b] for b in range(n)]
    own_sem,csend,crecv,send_sem,recv_sem=refs[5*n+1:]
    at=place(sizes)
    greet(at,sizes)
    R,N=outs[0].shape
    started=[]
    other=device(peer(at,sizes,"c",1))
    def pair_copies(b):
        return [pltpu.make_async_remote_copy(src_ref=grads[b][t].at[:,:,1-at["c"]],dst_ref=held[b].at[t],
            send_sem=csend.at[b,t],recv_sem=crecv.at[b,t],device_id=other,device_id_type=MESH) for t in range(T)]
    def own_copies(b):
        return [pltpu.make_async_copy(grads[b][t].at[:,:,at["c"]],own.at[b%2,t],own_sem.at[b%2,t]) for t in range(T)]
    def where(b,phase):
        done=orders[b][:phase]
        return tuple(at[a] if a in done else slice(None) for a in "tzx")
    def copies(b,phase):
        axis=orders[b][phase]
        made=[]
        for step in range(1,sizes[axis]):
            to=peer(at,sizes,axis,step)
            done=orders[b][:phase]
            src=tuple(at[a] if a in done else (to[axis] if a==axis else slice(None)) for a in "tzx")
            made.append(pltpu.make_async_remote_copy(src_ref=held[b].at[src],dst_ref=got[b][phase].at[step-1],
                send_sem=send_sem.at[b,phase,step-1],recv_sem=recv_sem.at[b,phase,step-1],
                device_id=device(to),device_id_type=MESH))
        return made
    def add_pair(b):
        def body(i,_):
            t,z,x=i//(Z*X),(i//X)%Z,i%X
            held[b][t,z,x]=(held[b][t,z,x].astype(F32)+own[b%2,t,z,x].astype(F32)).astype(BF)
            return 0
        lax.fori_loop(0,T*Z*X,body,0)
    def add(b,phase):
        axis=orders[b][phase]; done=orders[b][:phase+1]
        rest=[a for a in "tzx" if a not in done]
        if phase==2:
            total=held[b][at["t"],at["z"],at["x"]].astype(F32)
            for s in range(sizes[axis]-1): total=total+got[b][2][s].astype(F32)
            outs[b][...]=total
            return
        count=math.prod(sizes[a] for a in rest)
        def body(i,_):
            idx=dict(at); left=i
            for a in reversed(rest):
                idx[a]=lax.rem(left,sizes[a]); left=left//sizes[a]
            k=tuple(idx[a] for a in "tzx")
            total=held[b][k].astype(F32)
            for s in range(sizes[axis]-1): total=total+got[b][phase][(s,)+tuple(idx[a] for a in rest)].astype(F32)
            held[b][k]=total.astype(BF)
            return 0
        lax.fori_loop(0,count,body,0)
    for b in range(n):
        for cp in pair_copies(b): cp.start()
    pairs=[range(b,min(b+2,n)) for b in range(0,n,2)]
    def start(b,phase):
        for cp in copies(b,phase): cp.start()
    def arrive(b,phase):
        for cp in copies(b,phase): cp.wait()
        add(b,phase)
    def enter(pair):
        for b in pair:
            for cp in own_copies(b): cp.wait()
            for cp in pair_copies(b): cp.wait()
            add_pair(b)
            start(b,0)
    def load(pair):
        for b in pair:
            for cp in own_copies(b): cp.start()
    load(pairs[0])
    enter(pairs[0])
    for k,pair in enumerate(pairs):
        if k+1<len(pairs):
            load(pairs[k+1]); enter(pairs[k+1])
        for b in pair:
            arrive(b,0); start(b,1)
        for b in pair:
            arrive(b,1); start(b,2)
        if k>0:
            for b in pairs[k-1]: arrive(b,2)
    for b in pairs[-1]: arrive(b,2)

def reduce_rows(grads, sizes, orders, cid):
    n=len(grads); T,Z,X=sizes["t"],sizes["z"],sizes["x"]
    R,N=grads[0][0].shape[-2:]
    most=max(sizes.values())-1
    def got_shapes(order):
        dims=dict(t=T,z=Z,x=X); out=[]
        rest="tzx"
        for a in order:
            rest=[q for q in rest if q!=a]
            out.append(pltpu.VMEM((sizes[a]-1,)+tuple(dims[q] for q in rest)+(R,N),BF))
        return out
    scratch=[pltpu.VMEM((2,T,Z,X,R,N),BF)]+[pltpu.VMEM((T,Z,X,R,N),BF)]*n
    for o in orders: scratch+=got_shapes(o)
    scratch+=[pltpu.SemaphoreType.DMA((2,T)),pltpu.SemaphoreType.DMA((n,T)),pltpu.SemaphoreType.DMA((n,T)),
              pltpu.SemaphoreType.DMA((n,3,most)),pltpu.SemaphoreType.DMA((n,3,most))]
    return pl.pallas_call(
        lambda *refs: reduce_kernel(*refs,sizes=sizes,orders=orders),
        in_specs=[ANY]*(n*T), out_specs=[pl.BlockSpec(memory_space=pltpu.VMEM)]*n,
        out_shape=[jax.ShapeDtypeStruct((R,N),F32)]*n,
        scratch_shapes=scratch,
        compiler_params=pltpu.CompilerParams(collective_id=cid,has_side_effects=True,vmem_limit_bytes=60<<20),
        name="reduce_rows")(*[g for block in grads for g in block])


HEAD = 72
FAR = -1000000000.0
epsilon = 1e-06


def dg(a, b, ca, cb):
    return lax.dot_general(a, b, (((ca,), (cb,)), ((), ())), preferred_element_type=F32)


def join(refs):
    parts = [r[0] for r in refs]
    return parts[0] if len(parts) == 1 else jnp.concatenate(parts, axis=1)


def attend_kernel(limit, q, *refs, root, parts, masked):
    k, v, (o, lse) = join(refs[:parts]), join(refs[parts : 2 * parts]), refs[2 * parts :]
    s = dg(k, q[0], 0, 0) * root
    if masked:
        s = jnp.where(lax.broadcasted_iota(jnp.int32, s.shape, 0) < limit[0], s, FAR)
    m = jnp.max(s, axis=0, keepdims=True)
    p = jnp.exp(s - m)
    total = jnp.sum(p, axis=0, keepdims=True)
    low = (p * (1.0 / total)).astype(BF)
    o[0] = dg(v, low, 1, 0).astype(BF)
    lse[0] = m + jnp.log(total)


def head_spec(rows, cols):
    return pl.BlockSpec((1, rows, cols), lambda h, limit: (h, 0, 0))


def attend(limit, q, ks, vs, masked):
    H, E, Q = q.shape
    K = ks[0].shape[2]
    n = len(ks)
    work = H * E * Q * K * n
    return pl.pallas_call(
        lambda *r: attend_kernel(*r, root=1.0 / math.sqrt(E), parts=n, masked=masked),
        grid_spec=pltpu.PrefetchScalarGridSpec(
            num_scalar_prefetch=1,
            grid=(H,),
            in_specs=[head_spec(E, Q)] + [head_spec(E, K)] * (2 * n),
            out_specs=[head_spec(E, Q), head_spec(1, Q)],
        ),
        out_shape=[jax.ShapeDtypeStruct((H, E, Q), BF), jax.ShapeDtypeStruct((H, 1, Q), F32)],
        cost_estimate=pl.CostEstimate(flops=12 * work, bytes_accessed=8 * H * E * Q, transcendentals=H * Q * K * n),
        compiler_params=pltpu.CompilerParams(vmem_limit_bytes=48 << 20),
        name="attend",
    )(limit, q, *ks, *vs)


def attend_back_kernel(limit, q, g, lse, *refs, root, parts, masked):
    k, v = join(refs[:parts]), join(refs[parts : 2 * parts])
    dq, dks, dvs = refs[2 * parts], refs[2 * parts + 1 : 3 * parts + 1], refs[3 * parts + 1 :]
    s = dg(k, q[0], 0, 0) * root
    if masked:
        s = jnp.where(lax.broadcasted_iota(jnp.int32, s.shape, 0) < limit[0], s, FAR)
    p = jnp.exp(s - lse[0])
    dp = dg(v, g[0], 0, 0)
    delta = jnp.sum(p * dp, axis=0, keepdims=True)
    ds = (p * (dp - delta)).astype(BF)
    dv = dg(g[0], p.astype(BF), 1, 1).astype(BF)
    dk = (dg(q[0], ds, 1, 1) * root).astype(BF)
    width = dv.shape[1] // parts
    for i in range(parts):
        dvs[i][0] = dv[:, i * width : (i + 1) * width]
        dks[i][0] = dk[:, i * width : (i + 1) * width]
    dq[0] = (dg(k, ds, 1, 0) * root).astype(BF)


def attend_back(limit, q, g, lse, ks, vs, masked):
    H, E, Q = q.shape
    K = ks[0].shape[2]
    n = len(ks)
    work = H * E * Q * K * n
    out = pl.pallas_call(
        lambda *r: attend_back_kernel(*r, root=1.0 / math.sqrt(E), parts=n, masked=masked),
        grid_spec=pltpu.PrefetchScalarGridSpec(
            num_scalar_prefetch=1,
            grid=(H,),
            in_specs=[head_spec(E, Q), head_spec(E, Q), head_spec(1, Q)] + [head_spec(E, K)] * (2 * n),
            out_specs=[head_spec(E, Q)] + [head_spec(E, K)] * (2 * n),
        ),
        out_shape=[jax.ShapeDtypeStruct((H, E, Q), BF)] + [jax.ShapeDtypeStruct((H, E, K), BF)] * (2 * n),
        cost_estimate=pl.CostEstimate(flops=30 * work, bytes_accessed=8 * H * E * Q, transcendentals=H * Q * K * n),
        compiler_params=pltpu.CompilerParams(vmem_limit_bytes=48 << 20),
        name="attend_back",
    )(limit, q, g, lse, *ks, *vs)
    return out[0], out[1 : n + 1], out[n + 1 :]


def modulate(values, scale_in, shift_in):
    row_mean = jnp.mean(values, axis=-1, keepdims=True)
    centred = values - row_mean
    spread = jnp.mean(centred * centred, axis=-1, keepdims=True)
    return centred * lax.rsqrt(spread + epsilon) * (1.0 + scale_in) + shift_in


def gelu_tanh(values):
    return jax.nn.gelu(values, approximate=True)


def mm(spec, *operands):
    return jnp.einsum(spec, *operands, preferred_element_type=F32)


def swap(blocks, sizes):
    B, T = blocks.shape[0], sizes["t"]
    highs = sizes["z"] * sizes["x"]
    dp, t = lax.axis_index("dp"), lax.axis_index("tensor")
    c = dp % 2
    out = blocks
    for turn in range(B):
        pairs = []
        for high in range(highs):
            for core in range(2):
                for part in range(T):
                    to_t, to_c = core * B + (turn + part) % B, part // B
                    if (to_t, to_c) != (part, core):
                        pairs.append(((high * 2 + core) * T + part, (high * 2 + to_c) * T + to_t))
        j = lax.rem(turn + t, B)
        piece = blocks[0] if B == 1 else lax.dynamic_index_in_dim(blocks, j, 0, False)
        moved = lax.ppermute(piece, ("dp", "tensor"), pairs)
        stays = (c * B + j == t) & (t // B == c)
        got = jnp.where(stays, piece, moved)
        if B == 1:
            out = got[None]
        else:
            out = lax.dynamic_update_index_in_dim(out, got, lax.rem(t + B - turn, B), 0)
    return out


def to_partner(value, sizes):
    count = sizes["z"] * sizes["x"] * 2
    return lax.ppermute(value, "dp", [(i, i ^ 1) for i in range(count)])


def total_all(value, sizes):
    count = sizes["z"] * sizes["x"] * 2
    for name, size in (("dp", count), ("tensor", sizes["t"])):
        step = 1
        while step < size:
            value = value + lax.ppermute(value, name, [(i, i ^ step) for i in range(size)])
            step *= 2
    return value


def shards(
    latents, timestep, text, lengths, table, w_qkv, b_qv, w_proj, w_cq, w_ckv, b_cqv, w_cproj,
    w_fc1, b_fc1, w_fc2, b_out, cotangent, *, sizes,
):
    T = sizes["t"]
    B, n_rows, D = latents.shape
    R, _, w = w_qkv.shape
    N = 2 * w
    S = B * n_rows
    captions = text.shape[1]
    padded = -(-captions // 128) * 128
    t = lax.axis_index("tensor")
    c = lax.axis_index("dp") % 2
    near = ["zxtc", "ztxc"] * 4
    blocks = [
        w_qkv[:, :2].reshape(R, N),
        jnp.concatenate([w_qkv[:, 2], w_proj], axis=1),
        jnp.concatenate([w_cq, w_cproj], axis=1),
        w_ckv.reshape(R, N),
        w_fc1[:, :N], w_fc1[:, N:], w_fc2[:, :N], w_fc2[:, N:],
    ]
    whole = [g.reshape(T, D, N) for g in gather(blocks, sizes, near, 0)]
    tensors = range(T)
    W_qk = [whole[0][i] for i in tensors]
    W_v = [whole[1][i, :, :w] for i in tensors]
    W_proj = [whole[1][i, :, w:] for i in tensors]
    W_cq = [whole[2][i, :, :w] for i in tensors]
    W_cproj = [whole[2][i, :, w:] for i in tensors]
    W_ckv = [whole[3][i] for i in tensors]
    W_1 = [whole[4 + h][i] for i in tensors for h in range(2)]
    W_2 = [whole[6 + h][i] for i in tensors for h in range(2)]

    source = swap(latents, sizes).reshape(S, D).astype(F32)
    upstream = swap(cotangent, sizes).reshape(S, D).astype(F32)
    mine = c == t // B
    pick = lambda v: v[0] if B == 1 else lax.dynamic_index_in_dim(v, t % B, 0, False)
    words = pick(text)
    words = jnp.where(mine, words, to_partner(words, sizes))
    words = jnp.pad(words, ((0, padded - captions), (0, 0)))
    row = jnp.broadcast_to(pick(lengths).astype(F32), (2, D))
    stamp = jnp.concatenate([pick(timestep), row], axis=0)
    stamp = jnp.where(mine, stamp, to_partner(stamp, sizes))
    limit = stamp[6, :1].astype(jnp.int32)
    modulation = table + stamp[:6]
    shift_a, scale_a, gate_a, shift_m, scale_m, gate_m = (modulation[i : i + 1] for i in range(6))

    heads = lambda v: v.reshape(-1, HEAD, v.shape[-1])
    flat = lambda v: v.reshape(T, w, v.shape[-1])
    stacked = lambda parts: jnp.concatenate(parts, axis=0)
    out_rows = lambda v, W: sum(mm("ns,dn->sd", v[i], W[i]) for i in tensors)
    in_rows = lambda v, W: stacked([mm("dn,sd->ns", W[i], v) for i in tensors])

    normed_full, norm_back_a = jax.vjp(modulate, source, scale_a, shift_a)
    h_a = normed_full.astype(BF)
    qk = [mm("dn,sd->ns", W_qk[i], h_a) for i in tensors]
    q = heads((stacked([p[:w] for p in qk]) + b_qv[0][:, None]).astype(BF))
    k = heads(stacked([p[w:] for p in qk]).astype(BF))
    v = heads((in_rows(h_a, W_v) + b_qv[1][:, None]).astype(BF))
    k_far, v_far = to_partner(k, sizes), to_partner(v, sizes)
    mixed, lse = attend(limit, q, [k, k_far], [v, v_far], False)
    mixed_f = flat(mixed)
    attn = out_rows(mixed_f, W_proj) + b_out[0]
    after_self = source + gate_a * attn
    cross_in = after_self.astype(BF)
    cq = heads((in_rows(cross_in, W_cq) + b_cqv[0][:, None]).astype(BF))
    ckv = [mm("dn,kd->nk", W_ckv[i], words) for i in tensors]
    ck = heads(stacked([p[:w] for p in ckv]).astype(BF))
    cv = heads((stacked([p[w:] for p in ckv]) + b_cqv[1][:, None]).astype(BF))
    c_mixed, c_lse = attend(limit, cq, [ck], [cv], True)
    c_mixed_f = flat(c_mixed)
    after_cross = after_self + (out_rows(c_mixed_f, W_cproj) + b_out[1])
    normed_full, norm_back_m = jax.vjp(modulate, after_cross, scale_m, shift_m)
    h_m = normed_full.astype(BF)
    active, gelu_back = [], []
    for i, W in enumerate(W_1):
        pre = mm("sd,dn->sn", h_m, W) + b_fc1[i * N : (i + 1) * N]
        full, back = jax.vjp(gelu_tanh, pre)
        active.append(full.astype(BF))
        gelu_back.append(back)
    mlp = sum(mm("sn,dn->sd", a, W) for a, W in zip(active, W_2)) + b_out[2]
    block_out = swap((after_cross + gate_m * mlp).reshape(B, n_rows, D), sizes)

    g_mlp = (gate_m * upstream).astype(BF)
    g_gate_m = jnp.sum(upstream * mlp, axis=0)
    grad_2 = [mm("sd,sn->dn", g_mlp, a).astype(BF) for a in active]
    g_pre = [back(mm("sd,dn->sn", g_mlp, W))[0].astype(BF) for back, W in zip(gelu_back, W_2)]
    grad_1 = [mm("sd,sn->dn", h_m, g).astype(BF) for g in g_pre]
    g_b_fc1 = jnp.concatenate([jnp.sum(g, axis=0, dtype=F32) for g in g_pre])
    g_hm = sum(mm("sn,dn->sd", g, W) for g, W in zip(g_pre, W_1))
    g_norm, g_scale_m, g_shift_m = norm_back_m(g_hm)
    g_after_cross = upstream + g_norm
    g_cross = g_after_cross.astype(BF)
    grad_cproj = [mm("sd,ns->dn", g_cross, c_mixed_f[i]).astype(BF) for i in tensors]
    g_c_mixed = heads(in_rows(g_cross, W_cproj).astype(BF))
    g_cq, (g_ck,), (g_cv,) = attend_back(limit, cq, g_c_mixed, c_lse, [ck], [cv], True)
    g_cq_f, g_ck_f, g_cv_f = flat(g_cq), flat(g_ck), flat(g_cv)
    grad_cq = [mm("sd,ns->dn", cross_in, g_cq_f[i]).astype(BF) for i in tensors]
    g_ckv = [jnp.concatenate([g_ck_f[i], g_cv_f[i]], axis=0) for i in tensors]
    grad_ckv = [mm("kd,nk->dn", words, g_ckv[i]).astype(BF) for i in tensors]
    g_text = sum(mm("nk,dn->kd", g_ckv[i], W_ckv[i]) for i in tensors)
    g_b_cq = jnp.sum(g_cq, axis=2, dtype=F32).reshape(D)
    g_b_cv = jnp.sum(g_cv, axis=2, dtype=F32).reshape(D)
    g_after_self = g_after_cross + out_rows(g_cq_f, W_cq)
    g_attn = (gate_a * g_after_self).astype(BF)
    g_gate_a = jnp.sum(g_after_self * attn, axis=0)
    grad_proj = [mm("sd,ns->dn", g_attn, mixed_f[i]).astype(BF) for i in tensors]
    g_mixed = heads(in_rows(g_attn, W_proj).astype(BF))
    g_q, (g_k, g_k_far), (g_v, g_v_far) = attend_back(limit, q, g_mixed, lse, [k, k_far], [v, v_far], False)
    g_k = (g_k.astype(F32) + to_partner(g_k_far, sizes).astype(F32)).astype(BF)
    g_v = (g_v.astype(F32) + to_partner(g_v_far, sizes).astype(F32)).astype(BF)
    g_q_f, g_k_f, g_v_f = flat(g_q), flat(g_k), flat(g_v)
    g_qk = [jnp.concatenate([g_q_f[i], g_k_f[i]], axis=0) for i in tensors]
    grad_qk = [mm("sd,ns->dn", h_a, g_qk[i]).astype(BF) for i in tensors]
    grad_v = [mm("sd,ns->dn", h_a, g_v_f[i]).astype(BF) for i in tensors]
    g_b_q = jnp.sum(g_q, axis=2, dtype=F32).reshape(D)
    g_b_v = jnp.sum(g_v, axis=2, dtype=F32).reshape(D)
    g_ha = out_rows(g_qk, W_qk) + out_rows(g_v_f, W_v)
    g_norm, g_scale_a, g_shift_a = norm_back_a(g_ha)
    latents_grad = swap((g_after_self + g_norm).reshape(B, n_rows, D), sizes)

    beside = lambda a, b: [jnp.concatenate([x, y], axis=1) for x, y in zip(a, b)]
    rows = lambda parts: [p.reshape(sizes["z"], sizes["x"], 2, R, N) for p in parts]
    late = ["txz", "xtz"] * 2
    fc = reduce_rows(
        [rows(grad_2[0::2]), rows(grad_2[1::2]), rows(grad_1[0::2]), rows(grad_1[1::2])], sizes, late, 1
    )
    squares = reduce_rows(
        [rows(grad_ckv), rows(beside(grad_cq, grad_cproj)), rows(beside(grad_v, grad_proj)), rows(grad_qk)],
        sizes, late, 2,
    )
    o_ckv, o_cc, o_vp, o_qk = squares
    o_w_qkv = jnp.stack([o_qk[:, :w], o_qk[:, w:], o_vp[:, :w]], axis=1)
    o_w_ckv = jnp.stack([o_ckv[:, :w], o_ckv[:, w:]], axis=1)
    o_fc2 = jnp.concatenate(fc[:2], axis=1)
    o_fc1 = jnp.concatenate(fc[2:], axis=1)

    stamps = jnp.concatenate(
        [g_shift_a, g_scale_a, g_gate_a[None], g_shift_m, g_scale_m, g_gate_m[None]], axis=0
    )
    small = jnp.concatenate([g_text[:captions], stamps, jnp.zeros((2, D), F32)], axis=0)
    half = D // 2
    here = lax.dynamic_slice_in_dim(small, c * half, half, 1)
    there = lax.dynamic_slice_in_dim(small, (1 - c) * half, half, 1)
    here = here + to_partner(there, sizes)
    here = swap(here.reshape(captions + 8, B, half // B).transpose(1, 0, 2), sizes)
    sums = jnp.concatenate(
        [
            jnp.stack([g_b_q, g_b_v, g_b_cq, g_b_cv]),
            jnp.stack(
                [
                    jnp.sum(gate_a * g_after_self, axis=0),
                    jnp.sum(g_after_cross, axis=0),
                    jnp.sum(gate_m * upstream, axis=0),
                ]
            ),
            stamps,
            g_b_fc1.reshape(-1, D),
        ],
        axis=0,
    )
    sums = total_all(sums, sizes)
    return (
        block_out,
        latents_grad,
        here[:, captions : captions + 6],
        here[:, :captions],
        sums[7:13],
        o_w_qkv,
        sums[0:2],
        o_vp[:, w:],
        o_cc[:, :w],
        o_w_ckv,
        sums[2:4],
        o_cc[:, w:],
        o_fc1,
        sums[13:].reshape(-1),
        o_fc2,
        sums[4:7],
    )


def solution(mesh):
    sizes = {"t": mesh.shape["tensor"], "z": mesh.shape["dp"] // 4, "x": 2, "c": 2}
    split = P("dp", "tensor")
    kinds = P("dp", None, "tensor")
    tokens = P("dp", "tensor", None)
    return jax.shard_map(
        lambda *args: shards(*args, sizes=sizes),
        mesh=mesh,
        in_specs=(
            tokens, P("dp", None, None), P("dp", None, None), P("dp"), P(), kinds, P(), split, split, kinds,
            P(), split, split, P(), split, P(), tokens,
        ),
        out_specs=(
            tokens, tokens, kinds, kinds, P(), kinds, P(), split, split, kinds, P(), split, split, P(), split, P(),
        ),
        check_vma=False,
    )
```
